256 devices in a mesh: rep: 1, dp: 256 (over x, y, z, core).
Axes of the slice: x: 4, y: 4, z: 8, core: 2. Of those that a mesh axis runs over, the one named last changes fastest.
Arguments:
- x: bfloat16 [256, 1024, 768], P(('rep', 'dp'))
- dy: bfloat16 [256, 1024, 768], P(('rep', 'dp'))
- w_gate: bfloat16 [2, 768, 2048], replicated
- w_up: bfloat16 [2, 768, 2048], replicated
- w_down: bfloat16 [2, 2048, 768], replicated
- m_w_gate: float32 [2, 768, 2048], replicated
- m_w_up: float32 [2, 768, 2048], replicated
- m_w_down: float32 [2, 2048, 768], replicated
- v_w_gate: float32 [2, 768, 2048], replicated
- v_w_up: float32 [2, 768, 2048], replicated
- v_w_down: float32 [2, 2048, 768], replicated
Outputs:
- output 1: bfloat16 [2, 768, 2048], P('rep')
- output 2: bfloat16 [2, 768, 2048], P('rep')
- output 3: bfloat16 [2, 2048, 768], P('rep')
- output 4: float32 [2, 768, 2048], P('rep')
- output 5: float32 [2, 768, 2048], P('rep')
- output 6: float32 [2, 2048, 768], P('rep')
- output 7: float32 [2, 768, 2048], P('rep')
- output 8: float32 [2, 768, 2048], P('rep')
- output 9: float32 [2, 2048, 768], P('rep')
All inputs are finite; a program needn't handle non-finite values.
Results may differ from the reference program's by a relative error of at most 0.022.
Values are sent between devices in bfloat16 or wider.
A program may use at most 768 MiB of HBM per device.

```python
import jax
import jax.numpy as jnp
from jax import lax

SEQUENCES = 256
TOKENS = 1024
D = 768
FF = 2048
LAYERS = 2
NAMES = ("w_gate", "w_up", "w_down")
SHAPES = {"w_gate": (LAYERS, D, FF), "w_up": (LAYERS, D, FF), "w_down": (LAYERS, FF, D)}


def bump(key, n, height):
    away = (jnp.arange(n, dtype=jnp.int32) - jax.random.randint(key, (), 0, n, jnp.int32)) % n
    return jnp.where(away < n // 8, height, 1.0)


def together(key, own, strength):
    shared = jax.random.normal(key, own.shape[1:], jnp.float32)
    return (own + strength * shared) * lax.rsqrt(1 + strength * strength)


def setup_inputs(seed: int = 0, part: int = 0) -> dict:
    kx, kdy, ka, kb, kz, kf, kh, kl, *keys = jax.random.split(jax.random.key(seed), 8 + 3 * len(NAMES))
    kx, kdy, ka, kb = (jax.random.fold_in(k, part) for k in (kx, kdy, ka, kb))
    kw, km, kv = (keys[i::3] for i in range(3))
    shape = (SEQUENCES, TOKENS, D)
    much_x, much_dy = jax.random.uniform(kz, (2,), jnp.float32, 0.0, 1.0)
    loud = 2.0 ** jax.random.uniform(jax.random.fold_in(kz, 1), (), jnp.float32, -1.0, 2.0)
    layers = 2.0 ** jax.random.uniform(kl, (LAYERS, 1, 1), jnp.float32, -1.0, 1.0)
    x = together(ka, jax.random.normal(kx, shape, jnp.float32), much_x) * bump(kf, D, 4.0)
    dy = together(kb, jax.random.normal(kdy, shape, jnp.float32), much_dy)
    drawn = {"x": x.astype(jnp.bfloat16), "dy": (loud * dy * (SEQUENCES * TOKENS) ** -0.5).astype(jnp.bfloat16)}
    for key, name in zip(kw, NAMES, strict=True):
        w = jax.random.normal(key, SHAPES[name], jnp.float32) * SHAPES[name][1] ** -0.5
        drawn[name] = (w * {"w_gate": 1.0, "w_up": bump(kh, FF, 4.0), "w_down": layers}[name]).astype(jnp.bfloat16)
    for key, name in zip(km, NAMES, strict=True):
        drawn[f"m_{name}"] = 0.1 * jax.random.normal(key, SHAPES[name], jnp.float32)
    for key, name in zip(kv, NAMES, strict=True):
        drawn[f"v_{name}"] = loud * loud * jax.random.uniform(key, SHAPES[name], jnp.float32, 0.05, 0.15)
    return drawn


def matmul(a, w):
    return jnp.dot(a, w, preferred_element_type=jnp.float32).astype(jnp.bfloat16)


def normed(h):
    wide = h.astype(jnp.float32)
    scale = lax.rsqrt(jnp.mean(wide**2, -1, keepdims=True) + 1e-6)
    return (wide * scale).astype(jnp.bfloat16)


def layer(h, w):
    a = normed(h)
    gate = jnp.dot(a, w["w_gate"], preferred_element_type=jnp.float32)
    up = jnp.dot(a, w["w_up"], preferred_element_type=jnp.float32)
    return h + matmul((jax.nn.silu(gate) * up).astype(jnp.bfloat16), w["w_down"])


def adamw(w, m, v, g):
    m = 0.9 * m + 0.1 * g
    v = 0.95 * v + 0.05 * g * g
    step = m * lax.rsqrt(v + 1e-8) + 0.1 * w
    return (w - 0.02 * step).astype(jnp.bfloat16), m, v


def stack(weights, h):
    return lax.scan(lambda h, w: (layer(h, w), None), h, weights)[0]


def reference(x, dy, w_gate, w_up, w_down, m_w_gate, m_w_up, m_w_down, v_w_gate, v_w_up, v_w_down):
    weights = dict(zip(NAMES, (w_gate, w_up, w_down), strict=True))

    def take(so_far, sequence):
        h, by_y = sequence
        _, back = jax.vjp(lambda w: stack(w, h), weights)
        return jax.tree.map(lambda total, term: total + term.astype(jnp.float32), so_far, back(by_y)[0]), None

    none_yet = {name: jnp.zeros(w.shape, jnp.float32) for name, w in weights.items()}
    by_weights, _ = lax.scan(take, none_yet, (x, dy))
    gradients = [by_weights[name].astype(jnp.bfloat16).astype(jnp.float32) for name in NAMES]
    new = [
        adamw(w.astype(jnp.float32), m, v, g)
        for w, m, v, g in zip((w_gate, w_up, w_down), (m_w_gate, m_w_up, m_w_down), (v_w_gate, v_w_up, v_w_down), gradients, strict=True)
    ]
    return tuple(one[which] for which in range(3) for one in new)
```

```python
import functools

import jax
import jax.numpy as jnp
from jax import lax
from jax.experimental import pallas as pl
from jax.experimental.pallas import tpu as pltpu
from jax.sharding import PartitionSpec as P

NAMES = ("w_gate", "w_up", "w_down")
MESH = pl.DeviceIdType.MESH
F32, BF16 = jnp.float32, jnp.bfloat16
DIMS = (4, 4, 8)
ORDERS = ((0, 1, 2), (1, 2, 0), (2, 0, 1))
UNITS = 128
SHAPES = ((768, 2048), (768, 2048), (2048, 768))


def matmul(a, w):
    return jnp.dot(a, w, preferred_element_type=jnp.float32).astype(jnp.bfloat16)


def normed(h):
    wide = h.astype(jnp.float32)
    scale = lax.rsqrt(jnp.mean(wide**2, -1, keepdims=True) + 1e-6)
    return (wide * scale).astype(jnp.bfloat16)


def layer(h, w):
    a = normed(h)
    gate = jnp.dot(a, w["w_gate"], preferred_element_type=jnp.float32)
    up = jnp.dot(a, w["w_up"], preferred_element_type=jnp.float32)
    return h + matmul((jax.nn.silu(gate) * up).astype(jnp.bfloat16), w["w_down"])


def piece_scratch(kind):
    a, b, c = (DIMS[d] for d in ORDERS[kind])
    rows, cols = SHAPES[kind]
    u1, u2, u3 = UNITS // a, UNITS // a // b, UNITS // a // b // c
    dma = pltpu.SemaphoreType.DMA
    out = {
        "own": pltpu.VMEM((rows // 2, cols), BF16),
        "rec": pltpu.VMEM((rows // 2, cols), BF16),
        "acc1": pltpu.VMEM((u1, 48, 128), F32),
        "acc2": pltpu.VMEM((u2, 48, 128), F32),
        "core": dma((3,)),
    }
    if a > 1:
        out |= {
            "rs": pltpu.VMEM((2, a - 1, u1 // 2, 48, 128), BF16),
            "rr": pltpu.VMEM((2, a - 1, u1 // 2, 48, 128), BF16),
            "r_sem": dma((2, 2, a - 1)),
        }
    if b > 1:
        out |= {"bs": pltpu.VMEM((b - 1, u2, 48, 128), BF16), "br": pltpu.VMEM((b - 1, u2, 48, 128), BF16), "b_sem": dma((2, b - 1))}
    if c > 1:
        out |= {"cs": pltpu.VMEM((c - 1, u3, 48, 128), BF16), "cr": pltpu.VMEM((c - 1, u3, 48, 128), BF16), "c_sem": dma((2, c - 1))}
    return out


class Place:
    def __init__(self):
        self.me = lax.axis_index("dp")
        nx, ny, nz = DIMS
        self.core = lax.rem(self.me, 2)
        self.at = (self.me // (2 * ny * nz), lax.rem(self.me // (2 * nz), ny), lax.rem(self.me // 2, nz))
        self.stride = (2 * ny * nz, 2 * nz, 2)

    def peer(self, dim, away):
        n = DIMS[dim]
        return self.me + (lax.rem(self.at[dim] + away, n) - self.at[dim]) * self.stride[dim]

    def partner(self):
        return self.me + 1 - 2 * self.core


def remote(src, dst, send, recv, device):
    return pltpu.make_async_remote_copy(
        src_ref=src, dst_ref=dst, send_sem=send, recv_sem=recv, device_id={"dp": device}, device_id_type=MESH
    )


def gather_half(kind, s, unit, count, arrived, dst, base):
    own, rec = s["own"], s["rec"]
    if kind < 2:
        row0 = (unit // 16) * 48

        def body(q, _):
            row = pl.multiple_of(row0 + q * 16, 16)
            block, sub = q // 3, pl.multiple_of(lax.rem(q, 3) * 16, 16)
            for col in range(16):
                lanes = slice(col * 128, (col + 1) * 128)
                x = own[pl.ds(row, 16), lanes].astype(F32) + rec[pl.ds(row, 16), lanes].astype(F32)
                if arrived is not None:
                    x = x + arrived[block * 16 + col, pl.ds(sub, 16), :].astype(F32)
                dst[base + block * 16 + col, pl.ds(sub, 16), :] = x.astype(dst.dtype)
            return 0

        lax.fori_loop(0, count // 16 * 3, body, 0)
    else:
        row0 = (unit // 2) * 16

        def body(q, _):
            row = pl.multiple_of(row0 + q * 16, 16)
            for col in range(6):
                lanes, at, sub = slice(col * 128, (col + 1) * 128), 2 * q + col // 3, slice(col % 3 * 16, col % 3 * 16 + 16)
                x = own[pl.ds(row, 16), lanes].astype(F32) + rec[pl.ds(row, 16), lanes].astype(F32)
                if arrived is not None:
                    x = x + arrived[at, sub, :].astype(F32)
                dst[base + at, sub, :] = x.astype(dst.dtype)
            return 0

        lax.fori_loop(0, count // 2, body, 0)


def piece_stages(kind, g, out, s, here, started):
    da, db, dc = ORDERS[kind]
    a, b, c = DIMS[da], DIMS[db], DIMS[dc]
    u1, u2, u3 = UNITS // a, UNITS // a // b, UNITS // a // b // c
    half, rows = u1 // 2, SHAPES[kind][0] // 2
    state = {}

    def begin():
        other = pl.multiple_of((1 - here.core) * rows, 16)
        mine = pl.multiple_of(here.core * rows, 16)
        state["core"] = remote(g.at[pl.ds(other, rows)], s["rec"], s["core"].at[0], s["core"].at[1], here.partner())
        state["core"].start()
        started.append(state["core"])
        state["own"] = pltpu.make_async_copy(g.at[pl.ds(mine, rows)], s["own"], s["core"].at[2])
        state["own"].start()

    def ring_copy(way, step):
        to = here.peer(da, 1 if way == 0 else a - 1)
        return remote(s["rs"].at[way, step], s["rr"].at[way, step], s["r_sem"].at[0, way, step], s["r_sem"].at[1, way, step], to)

    def chunk(way, step):
        i = here.at[da]
        j = lax.rem(i + 2 * a - 1 - step, a) if way == 0 else lax.rem(i + 1 + step, a)
        return j * u1 + way * half

    def ring_send(way, step, arrived):
        gather_half(kind, s, chunk(way, step), half, arrived, s["rs"].at[way, step], 0)
        copy = ring_copy(way, step)
        copy.start()
        started.append(copy)
        state[way, step] = copy

    def first():
        state["own"].wait()
        state["core"].wait_recv()
        if a == 1:
            gather_half(kind, s, 0, u1, None, s["acc1"], 0)
            b_send()
        for way in range(2 if a > 1 else 0):
            ring_send(way, 0, None)

    def ring_step(step):
        for way in range(2):
            state[way, step].wait_recv()
            arrived = s["rr"].at[way, step]
            if step < a - 2:
                ring_send(way, step + 1, arrived)
            else:
                gather_half(kind, s, chunk(way, a - 1), half, arrived, s["acc1"], way * half)
        if step == a - 2:
            b_send()

    def direct_send(n, dim, units, acc, send, recv, sem, name):
        for d in range(1, n):
            j = lax.rem(here.at[dim] + d, n)

            def body(k, _, j=j, d=d):
                send[d - 1, k] = acc[j * units + k].astype(BF16)
                return 0

            lax.fori_loop(0, units, body, 0)
            copy = remote(send.at[d - 1], recv.at[d - 1], sem.at[0, d - 1], sem.at[1, d - 1], here.peer(dim, d))
            copy.start()
            started.append(copy)
            state[name, d] = copy

    def b_send():
        if b > 1:
            direct_send(b, db, u2, s["acc1"], s["bs"], s["br"], s["b_sem"], "b")

    def b_recv():
        for d in range(1, b):
            state["b", d].wait_recv()

        def body(k, _):
            x = s["acc1"][here.at[db] * u2 + k]
            for d in range(1, b):
                x = x + s["br"][d - 1, k].astype(F32)
            s["acc2"][k] = x
            return 0

        lax.fori_loop(0, u2, body, 0)
        if c > 1:
            direct_send(c, dc, u3, s["acc2"], s["cs"], s["cr"], s["c_sem"], "c")

    def c_recv():
        for d in range(1, c):
            state["c", d].wait_recv()

        def body(k, _):
            x = s["acc2"][here.at[dc] * u3 + k]
            for d in range(1, c):
                x = x + s["cr"][d - 1, k].astype(F32)
            out[k] = x.astype(BF16)
            return 0

        lax.fori_loop(0, u3, body, 0)

    stages = [begin, first] + [functools.partial(ring_step, step) for step in range(a - 1)] + [b_recv, c_recv]
    ring_us = 8.5 if a == 4 else 4.6
    return stages, ring_us


def scatter_kernel(kinds, names, *refs):
    pieces = len(kinds)
    grads, outs, scratch = refs[:pieces], refs[pieces : 2 * pieces], refs[2 * pieces :]
    here = Place()
    barrier = pltpu.get_barrier_semaphore()
    peers = [here.partner()] + [here.peer(dim, away) for dim in range(3) for away in range(1, DIMS[dim])]
    for peer in peers:
        pl.semaphore_signal(barrier, inc=1, device_id={"dp": peer}, device_id_type=MESH)
    pl.semaphore_wait(barrier, len(peers))

    order, started = [], []
    for n, kind in enumerate(kinds):
        s, scratch = dict(zip(names[n], scratch)), scratch[len(names[n]) :]
        stages, ring_us = piece_stages(kind, grads[n], outs[n], s, here, started)
        when = 3.0 + 2.6 * n
        for k, stage in enumerate(stages):
            order.append((0.1 * n - 100 if k == 0 else when, len(order), stage))
            if k >= 1:
                when += ring_us if k < len(stages) - 2 else 7.0
    for _, _, stage in sorted(order, key=lambda entry: entry[:2]):
        stage()
    for copy in started:
        copy.wait_send()


def reduce_scatter(grads, kinds):
    specs = [piece_scratch(kind) for kind in kinds]
    units = UNITS // (DIMS[0] * DIMS[1] * DIMS[2])
    return pl.pallas_call(
        functools.partial(scatter_kernel, kinds, [tuple(spec) for spec in specs]),
        out_shape=[jax.ShapeDtypeStruct((units, 48, 128), BF16)] * len(kinds),
        in_specs=[pl.BlockSpec(memory_space=pl.ANY)] * len(kinds),
        out_specs=[pl.BlockSpec(memory_space=pltpu.VMEM)] * len(kinds),
        scratch_shapes=[shape for spec in specs for shape in spec.values()],
        compiler_params=pltpu.CompilerParams(collective_id=0, has_side_effects=True, vmem_limit_bytes=60 * 2**20),
        cost_estimate=pl.CostEstimate(flops=50_000_000, bytes_accessed=30_000_000, transcendentals=0),
        name="reduce_scatter",
    )(*grads)


def adamw(w, m, v, g):
    m = 0.9 * m + 0.1 * g
    v = 0.95 * v + 0.05 * g * g
    step = m * lax.rsqrt(v + 1e-8) + 0.1 * w
    return (w - 0.02 * step).astype(BF16), m, v


def adamw_kernel(kind, g_ref, w_ref, m_ref, v_ref, *rest):
    new_w, new_m, new_v = rest[-3:]

    def tile(g, rows, lanes):
        at = (0, rows, lanes)
        new_w[at], new_m[at], new_v[at] = adamw(w_ref[at].astype(F32), m_ref[at], v_ref[at], g.astype(F32))

    order = ORDERS[kind]
    span = {0: (1, 2, 8), 1: (4, 1, 4), 2: (4, 4, 1)}[kind]
    units = []
    sizes = [span[d] for d in order]
    for i in range(sizes[0]):
        for j in range(sizes[1]):
            for k in range(sizes[2]):
                at = [0, 0, 0]
                at[order[0]], at[order[1]], at[order[2]] = i, j, k
                units.append(tuple(at))
    for n, (x, y, z) in enumerate(units):
        if kind < 2:
            tile(g_ref[x, y, z, 0], slice(None), slice(n * 128, (n + 1) * 128))
        else:
            for k in range(3):
                lane = (n % 2 * 3 + k) * 128
                tile(g_ref[x, y, z, 0, 16 * k : 16 * k + 16], slice(n // 2 * 16, n // 2 * 16 + 16), slice(lane, lane + 128))


def adamw_call(kind, number, g, w, m, v, before):
    rows, cols = SHAPES[kind]
    block = pl.BlockSpec((1, rows // 16, cols), lambda i: (number, i, 0))
    if kind == 0:
        g_spec = pl.BlockSpec((1, 2, 8, 1, 48, 128), lambda i: (i % 8 // 2, i % 2, 0, i // 8, 0, 0))
    elif kind == 1:
        g_spec = pl.BlockSpec((4, 1, 4, 1, 48, 128), lambda i: (0, i % 8 // 2, i % 2, i // 8, 0, 0))
    else:
        g_spec = pl.BlockSpec((4, 4, 1, 1, 48, 128), lambda i: (0, 0, i % 8, i // 8, 0, 0))
    before = before or ()
    return pl.pallas_call(
        functools.partial(adamw_kernel, kind),
        grid=(16,),
        out_shape=[jax.ShapeDtypeStruct(x.shape, x.dtype) for x in (w, m, v)],
        in_specs=[g_spec, block, block, block] + [pl.BlockSpec(memory_space=pl.ANY)] * len(before),
        out_specs=[block] * 3,
        input_output_aliases={4 + i: i for i in range(len(before))},
        compiler_params=pltpu.CompilerParams(dimension_semantics=("arbitrary",), vmem_limit_bytes=60 * 2**20),
        cost_estimate=pl.CostEstimate(flops=rows * cols * 200, bytes_accessed=rows * cols * 22, transcendentals=rows * cols),
        name=f"adamw_{NAMES[kind]}",
    )(g, w, m, v, *before)


def solution(mesh):
    def step(x, dy, *arrays):
        weights, m, v = (arrays[i : i + 3] for i in (0, 3, 6))
        layers = weights[0].shape[0]
        h, kept = x[0], []
        for number in range(layers):
            kept.append(h)
            h = layer(h, {name: w[number] for name, w in zip(NAMES, weights, strict=True)})
        by_h, grads = dy[0], {}
        for number in reversed(range(layers)):
            _, back = jax.vjp(lambda w, h: layer(h, w), {name: w[number] for name, w in zip(NAMES, weights, strict=True)}, kept[number])
            by_w, by_h = back(by_h)
            for kind, name in enumerate(NAMES):
                grads[number, kind] = by_w[name]
        keys = [(number, kind) for number in reversed(range(layers)) for kind in range(3)]
        shards = reduce_scatter([grads[key] for key in keys], [kind for _, kind in keys])
        new = [None] * 3
        for (number, kind), shard in zip(keys, shards):
            g = lax.all_gather(shard[0], "dp").reshape(*DIMS, 2, 48, 128)
            new[kind] = adamw_call(kind, number, g, weights[kind], m[kind], v[kind], new[kind])
        return tuple(one[which] for which in range(3) for one in new)

    return jax.shard_map(
        step,
        mesh=mesh,
        in_specs=(P(("rep", "dp"), None, None),) * 2 + (P(None, None, None),) * 9,
        out_specs=(P("rep", None, None),) * 9,
        check_vma=False,
    )
```

```python
import functools

import jax
import jax.numpy as jnp
from jax import lax
from jax.experimental import pallas as pl
from jax.experimental.pallas import tpu as pltpu
from jax.sharding import PartitionSpec as P

NAMES = ("w_gate", "w_up", "w_down")
MESH = pl.DeviceIdType.MESH
F32, BF16 = jnp.float32, jnp.bfloat16
DIMS = (4, 4, 8)
UNITS = 128
SHAPES = ((768, 2048), (768, 2048), (2048, 768))
ORDERS = (("x", "y", "z"), ("y", "x", "z"), ("z", "x", "y"), ("xy", "yx", "z"))
MINE = ((1, 0, 3), (0, 2, 2), (0, 1, 1), (0, 0, 0))


def matmul(a, w):
    return jnp.dot(a, w, preferred_element_type=jnp.float32).astype(jnp.bfloat16)


def normed(h):
    wide = h.astype(jnp.float32)
    scale = lax.rsqrt(jnp.mean(wide**2, -1, keepdims=True) + 1e-6)
    return (wide * scale).astype(jnp.bfloat16)


def layer(h, w):
    a = normed(h)
    gate = jnp.dot(a, w["w_gate"], preferred_element_type=jnp.float32)
    up = jnp.dot(a, w["w_up"], preferred_element_type=jnp.float32)
    return h + matmul((jax.nn.silu(gate) * up).astype(jnp.bfloat16), w["w_down"])


class Axis:
    def __init__(self, me, n, at, stride):
        self.me, self.n, self.at, self.stride = me, n, at, stride

    def peer(self, away):
        return self.me + (lax.rem(self.at + away, self.n) - self.at) * self.stride


class Place:
    def __init__(self):
        me = lax.axis_index("dp")
        nx, ny, nz = DIMS
        self.me, self.core = me, lax.rem(me, 2)
        x, y, z = me // (2 * ny * nz), lax.rem(me // (2 * nz), ny), lax.rem(me // 2, nz)
        sx, sy, core = 2 * ny * nz, 2 * nz, self.core
        self.axes = {"x": Axis(me, nx, x, sx), "y": Axis(me, ny, y, sy), "z": Axis(me, nz, z, 2)}
        self.axes["xy"] = Axis(me, nx, x + core * (y - x), sx + core * (sy - sx)) if nx == ny else self.axes["x"]
        self.axes["yx"] = Axis(me, ny, y + core * (x - y), sy + core * (sx - sy)) if nx == ny else self.axes["y"]
        self.partner = me + 1 - 2 * core


def sizes(order):
    nx, ny, nz = DIMS
    n = {"x": nx, "y": ny, "z": nz, "xy": nx, "yx": ny}
    return tuple(n[axis] for axis in ORDERS[order])


def piece_scratch(kind, order):
    a, b, c = sizes(order)
    rows, cols = SHAPES[kind]
    u1, u2, u3 = UNITS // a, UNITS // a // b, UNITS // a // b // c
    dma = pltpu.SemaphoreType.DMA
    out = {
        "own": pltpu.VMEM((rows // 2, cols), BF16),
        "rec": pltpu.VMEM((rows // 2, cols), BF16),
        "all": pltpu.VMEM((UNITS, 48, 128), BF16),
        "acc1": pltpu.VMEM((u1, 48, 128), F32),
        "acc2": pltpu.VMEM((u2, 48, 128), F32),
        "core": dma((3,)),
        "end": dma((3, 1 + 2 * max(a // 2, 1))),
    }
    for name, n, units in (("a", a, u1), ("b", b, u2)):
        if n > 1:
            out[name + "s"] = pltpu.VMEM((2, n // 2, units, 48, 128), BF16)
            out[name + "r"] = pltpu.VMEM((2, n // 2, units, 48, 128), BF16)
            out[name + "_sum"] = dma((2, 2, n // 2))
            out[name + "_all"] = dma((2, 2, n // 2))
    if c > 1:
        out |= {"cs": pltpu.VMEM((c - 1, u3, 48, 128), BF16), "cr": pltpu.VMEM((c - 1, u3, 48, 128), BF16)}
        out |= {"c_sum": dma((2, c - 1)), "c_all": dma((2, c - 1))}
    return out


def remote(src, dst, send, recv, device):
    return pltpu.make_async_remote_copy(
        src_ref=src, dst_ref=dst, send_sem=send, recv_sem=recv, device_id={"dp": device}, device_id_type=MESH
    )


def first_row(kind, unit):
    return pl.multiple_of((unit // 16) * 48 if kind < 2 else (unit // 2) * 16, 16)


def row_count(kind, count):
    return count // 16 * 48 if kind < 2 else count // 2 * 16


def tiles(kind, unit, count, tile):
    row0 = first_row(kind, unit)

    def body(q, _):
        rows = pl.ds(pl.multiple_of(row0 + q * 16, 16), 16)
        for col in range(16 if kind < 2 else 6):
            lanes = slice(col * 128, (col + 1) * 128)
            if kind < 2:
                tile(rows, lanes, q // 3 * 16 + col, pl.ds(pl.multiple_of(lax.rem(q, 3) * 16, 16), 16))
            else:
                tile(rows, lanes, 2 * q + col // 3, slice(col % 3 * 16, col % 3 * 16 + 16))
        return 0

    lax.fori_loop(0, row_count(kind, count) // 16, body, 0)


def piece_stages(kind, order, g, out, s, here, started):
    axes = [here.axes[name] for name in ORDERS[order]]
    a, b, c = sizes(order)
    u1, u2, u3 = UNITS // a, UNITS // a // b, UNITS // a // b // c
    rows = SHAPES[kind][0] // 2
    ia, ib, ic = (axis.at for axis in axes)
    base_b = ia * u1
    base_c = base_b + ib * u2
    base = base_c + ic * u3
    state = {}

    def go(key, copy):
        copy.start()
        started.append(copy.wait_send)
        state[key] = copy

    def begin():
        other = pl.multiple_of((1 - here.core) * rows, 16)
        mine = pl.multiple_of(here.core * rows, 16)
        go("core", remote(g.at[pl.ds(other, rows)], s["rec"], s["core"].at[0], s["core"].at[1], here.partner))
        state["own"] = pltpu.make_async_copy(g.at[pl.ds(mine, rows)], s["own"], s["core"].at[2])
        state["own"].start()

    def add_a(unit, count, arrived, dst, at):
        def tile(rows, lanes, n, sub):
            x = s["own"][rows, lanes].astype(F32) + s["rec"][rows, lanes].astype(F32)
            for ref, skip in arrived:
                x = x + ref[skip + n, sub, :].astype(F32)
            dst[at + n, sub, :] = x.astype(dst.dtype)

        tiles(kind, unit, count, tile)

    def add_b(unit, count, arrived, dst, at):
        def body(n, _):
            x = s["acc1"][unit + n]
            for ref, skip in arrived:
                x = x + ref[skip + n].astype(F32)
            dst[at + n] = x.astype(dst.dtype)
            return 0

        lax.fori_loop(0, count, body, 0)

    def chain(name, axis, units, add, acc):
        n, steps, half = axis.n, axis.n // 2, units // 2

        def send(way, t):
            far = steps - t
            j = lax.rem(axis.at + (far if way == 0 else n - far), n)
            buf = s[name + "s"].at[way, t]
            got = s[name + "r"].at[way, t - 1] if t > 0 else None
            long, short = way * half, (1 - way) * half
            add(j * units + long, half, [(got, long)] if t > 0 else [], buf, long)
            if t > 0:
                add(j * units + short, half, [(got, short)] if t > 1 else [], buf, short)
                src, dst = buf, s[name + "r"].at[way, t]
            else:
                src, dst = buf.at[pl.ds(long, half)], s[name + "r"].at[way, t, pl.ds(long, half)]
            sem = s[name + "_sum"]
            go((name, way, t), remote(src, dst, sem.at[0, way, t], sem.at[1, way, t], axis.peer(1 if way == 0 else n - 1)))

        def start():
            if n == 1:
                add(0, units, [], acc, 0)
                return
            for way in range(2):
                send(way, 0)

        def step(t):
            for way in range(2):
                state[name, way, t].wait_recv()
                if t + 1 < steps:
                    send(way, t + 1)
            if t + 1 == steps:
                up, down = s[name + "r"].at[0, t], s[name + "r"].at[1, t]
                j = axis.at * units
                add(j, half, [(up, 0)] + ([(down, 0)] if t > 0 else []), acc, 0)
                add(j + half, half, [(down, half)] + ([(up, half)] if t > 0 else []), acc, half)

        return start, step

    def c_start():
        for d in range(1, c):
            j = lax.rem(ic + d, c)
            for k in range(u3):
                s["cs"][d - 1, k] = s["acc2"][j * u3 + k].astype(BF16)
            sem = s["c_sum"]
            go(("c", d), remote(s["cs"].at[d - 1], s["cr"].at[d - 1], sem.at[0, d - 1], sem.at[1, d - 1], axes[2].peer(d)))

    def c_step():
        for d in range(1, c):
            state["c", d].wait_recv()
        for k in range(u3):
            x = s["acc2"][ic * u3 + k]
            for d in range(1, c):
                x = x + s["cr"][d - 1, k].astype(F32)
            s["all"][base + k] = x.astype(BF16)

    def c_all_start():
        mine = s["all"].at[pl.ds(base, u3)]
        for d in range(1, c):
            sem = s["c_all"]
            go(("c_all", d), remote(mine, mine, sem.at[0, d - 1], sem.at[1, d - 1], axes[2].peer(d)))

    def c_all_step():
        for d in range(1, c):
            state["c_all", d].wait_recv()

    def spread(name, axis, units, first):
        n, steps, half = axis.n, axis.n // 2, units // 2

        def part(way, t, chunk):
            whole = t + 1 < steps
            return first + chunk * units + (0 if whole else way * half), units if whole else half

        def send(way, t):
            unit, count = part(way, t, lax.rem(axis.at + (n - t if way == 0 else t), n))
            ref, sem = s["all"].at[pl.ds(unit, count)], s[name + "_all"]
            go((name + "_all", way, t), remote(ref, ref, sem.at[0, way, t], sem.at[1, way, t], axis.peer(1 if way == 0 else n - 1)))

        def start():
            for way in range(2 if n > 1 else 0):
                send(way, 0)

        def step(t, then=None):
            for way in range(2):
                state[name + "_all", way, t].wait_recv()
                if t + 1 < steps:
                    send(way, t + 1)
            for way in range(2 if then else 0):
                unit, count = part(way, t, lax.rem(axis.at + (n - 1 - t if way == 0 else 1 + t), n))
                then(unit, count, 1 + way * steps + t)

        return start, step

    def finish(unit, count, slot):
        def tile(rows, lanes, n, sub):
            s["own"][rows, lanes] = s["all"][unit + n, sub, :]

        tiles(kind, unit, count, tile)
        row, many = first_row(kind, unit), row_count(kind, count)
        src = s["own"].at[pl.ds(row, many)]
        dst = out.at[pl.ds(pl.multiple_of(here.core * rows + row, 16), many)]
        copy = remote(src, dst, s["end"].at[0, slot], s["end"].at[1, slot], here.partner)
        local = pltpu.make_async_copy(src, dst, s["end"].at[2, slot])
        copy.start()
        local.start()
        started.extend([copy.wait_send, copy.wait_recv, local.wait])

    a_start, a_step = chain("a", axes[0], u1, add_a, s["acc1"])
    b_start, b_step = chain("b", axes[1], u2, add_b, s["acc2"])
    b_all_start, b_all_step = spread("b", axes[1], u2, base_b)
    a_all_start, a_all_step = spread("a", axes[0], u1, 0)

    def join(*parts):
        def run():
            for part in parts:
                part()

        return run

    def wait_core():
        state["own"].wait()
        state["core"].wait_recv()

    def own_rows():
        finish(base_b, u1, 0)

    stages = [[wait_core, a_start]]
    times = [2.0]
    for t in range(a // 2):
        stages.append([functools.partial(a_step, t)])
        times.append({4: (7.0, 13.0)[t % 2], 8: 6.5}.get(a, 5.0))
    stages[-1].append(b_start)
    for t in range(b // 2):
        stages.append([functools.partial(b_step, t)])
        times.append(4.0)
    stages[-1].append(c_start)
    stages.append([c_step, c_all_start])
    times.append(4.5)
    stages.append([c_all_step, b_all_start])
    times.append(4.5)
    for t in range(b // 2):
        stages.append([functools.partial(b_all_step, t)])
        times.append(4.0)
    stages[-1] += [a_all_start, own_rows]
    for t in range(a // 2):
        stages.append([functools.partial(a_all_step, t, finish)])
        times.append({4: (13.0, 7.0)[t % 2], 8: 6.5}.get(a, 5.0))
    return begin, [(join(*stage), time) for stage, time in zip(stages, times)]


def sum_kernel(pieces, names, *refs):
    count = len(pieces)
    grads, outs, scratch = refs[:count], refs[count : 2 * count], refs[2 * count :]
    here = Place()
    barrier = pltpu.get_barrier_semaphore()
    axes = [here.axes[name] for name in "xyz"]
    peers = [here.partner] + [axis.peer(away) for axis in axes for away in range(1, axis.n)]
    for peer in peers:
        pl.semaphore_signal(barrier, inc=1, device_id={"dp": peer}, device_id_type=MESH)
    pl.semaphore_wait(barrier, len(peers))

    plan, started = [], []
    for n, (kind, order) in enumerate(pieces):
        s, scratch = dict(zip(names[n], scratch)), scratch[len(names[n]) :]
        begin, stages = piece_stages(kind, order, grads[n], outs[n], s, here, started)
        begin()
        when = 2.4 * n
        for stage, time in stages:
            when += time
            plan.append((when, len(plan), stage))
    for _, _, stage in sorted(plan, key=lambda entry: entry[:2]):
        stage()
    for wait in started:
        wait()


def group_sum(grads, pieces):
    specs = [piece_scratch(*piece) for piece in pieces]
    return pl.pallas_call(
        functools.partial(sum_kernel, pieces, [tuple(spec) for spec in specs]),
        out_shape=[jax.ShapeDtypeStruct(g.shape, BF16) for g in grads],
        in_specs=[pl.BlockSpec(memory_space=pl.ANY)] * len(pieces),
        out_specs=[pl.BlockSpec(memory_space=pl.ANY)] * len(pieces),
        scratch_shapes=[shape for spec in specs for shape in spec.values()],
        compiler_params=pltpu.CompilerParams(collective_id=0, has_side_effects=True, vmem_limit_bytes=60 * 2**20),
        cost_estimate=pl.CostEstimate(flops=300_000_000, bytes_accessed=60_000_000, transcendentals=0),
        name="group_sum",
    )(*grads)


def adamw(w, m, v, g):
    m = 0.9 * m + 0.1 * g
    v = 0.95 * v + 0.05 * g * g
    step = m * lax.rsqrt(v + 1e-8) + 0.1 * w
    return (w - 0.02 * step).astype(jnp.bfloat16), m, v


def solution(mesh):
    def step(x, dy, *arrays):
        weights, m, v = (arrays[i : i + 3] for i in (0, 3, 6))
        layers = weights[0].shape[0]
        h, kept = x[0], []
        for number in range(layers):
            kept.append(h)
            h = layer(h, {name: w[number] for name, w in zip(NAMES, weights, strict=True)})
        by_h, grads = dy[0], {}
        for number in reversed(range(layers)):
            _, back = jax.vjp(lambda w, h: layer(h, w), {name: w[number] for name, w in zip(NAMES, weights, strict=True)}, kept[number])
            by_w, by_h = back(by_h)
            for kind, name in enumerate(NAMES):
                grads[number, kind] = by_w[name]
        sums = {key: lax.psum(g, "dp") for key, g in grads.items() if key not in [piece[:2] for piece in MINE]}
        mine = group_sum([grads[piece[:2]] for piece in MINE], [piece[1:] for piece in MINE])
        sums |= {piece[:2]: g for piece, g in zip(MINE, mine)}
        gradients = [jnp.stack([sums[number, i] for number in range(layers)]).astype(F32) for i in range(3)]
        new = [adamw(w.astype(F32), m, v, g) for w, m, v, g in zip(weights, m, v, gradients, strict=True)]
        return tuple(one[which] for which in range(3) for one in new)

    return jax.shard_map(
        step,
        mesh=mesh,
        in_specs=(P(("rep", "dp"), None, None),) * 2 + (P(None, None, None),) * 9,
        out_specs=(P("rep", None, None),) * 9,
        check_vma=False,
    )
```

```python
import functools
import itertools

import jax
import jax.numpy as jnp
from jax import lax
from jax.experimental import pallas as pl
from jax.experimental.pallas import tpu as pltpu
from jax.sharding import PartitionSpec as P

NAMES = ("w_gate", "w_up", "w_down")
MESH = pl.DeviceIdType.MESH
F32, BF16 = jnp.float32, jnp.bfloat16
DIMS = (4, 4, 8)
LAYERS = 2
UNITS = 128
SHAPES = ((768, 2048), (768, 2048), (2048, 768))
ORDERS = (("x", "y", "z"), ("y", "x", "z"), ("z", "x", "y"), ("xy", "yx", "z"))
PIECES = ((2, 2), (0, 0), (1, 1))


def matmul(a, w):
    return jnp.dot(a, w, preferred_element_type=jnp.float32).astype(jnp.bfloat16)


def normed(h):
    wide = h.astype(jnp.float32)
    scale = lax.rsqrt(jnp.mean(wide**2, -1, keepdims=True) + 1e-6)
    return (wide * scale).astype(jnp.bfloat16)


def layer(h, w):
    a = normed(h)
    gate = jnp.dot(a, w["w_gate"], preferred_element_type=jnp.float32)
    up = jnp.dot(a, w["w_up"], preferred_element_type=jnp.float32)
    return h + matmul((jax.nn.silu(gate) * up).astype(jnp.bfloat16), w["w_down"])


class Axis:
    def __init__(self, me, n, at, stride):
        self.me, self.n, self.at, self.stride = me, n, at, stride

    def peer(self, away):
        return self.me + (lax.rem(self.at + away, self.n) - self.at) * self.stride


class Place:
    def __init__(self):
        me = lax.axis_index("dp")
        nx, ny, nz = DIMS
        self.me, self.core = me, lax.rem(me, 2)
        x, y, z = me // (2 * ny * nz), lax.rem(me // (2 * nz), ny), lax.rem(me // 2, nz)
        sx, sy, core = 2 * ny * nz, 2 * nz, self.core
        self.axes = {"x": Axis(me, nx, x, sx), "y": Axis(me, ny, y, sy), "z": Axis(me, nz, z, 2)}
        self.axes["xy"] = Axis(me, nx, x + core * (y - x), sx + core * (sy - sx)) if nx == ny else self.axes["x"]
        self.axes["yx"] = Axis(me, ny, y + core * (x - y), sy + core * (sx - sy)) if nx == ny else self.axes["y"]
        self.partner = me + 1 - 2 * core


def sizes(order):
    nx, ny, nz = DIMS
    n = {"x": nx, "y": ny, "z": nz, "xy": nx, "yx": ny}
    return tuple(n[axis] for axis in ORDERS[order])


def piece_scratch(kind, order):
    a, b, c = sizes(order)
    rows, cols = SHAPES[kind]
    u1, u2, u3 = UNITS // a, UNITS // a // b, UNITS // a // b // c
    dma = pltpu.SemaphoreType.DMA
    out = {
        "own": pltpu.VMEM((LAYERS, rows // 2, cols), BF16),
        "rec": pltpu.VMEM((LAYERS, rows // 2, cols), BF16),
        "all": pltpu.VMEM((UNITS, 96, 128), BF16),
        "acc1": pltpu.VMEM((u1, 96, 128), F32),
        "acc2": pltpu.VMEM((u2, 96, 128), F32),
        "core": dma((LAYERS, 3)),
        "end": dma((3, 1 + 2 * max(a // 2, 1))),
    }
    for name, n, units in (("a", a, u1), ("b", b, u2)):
        if n > 1:
            out[name + "s"] = pltpu.VMEM((2, n // 2, units, 96, 128), BF16)
            out[name + "r"] = pltpu.VMEM((2, n // 2, units, 96, 128), BF16)
            out[name + "_sum"] = dma((2, 2, n // 2))
            out[name + "_all"] = dma((2, 2, n // 2))
    if c > 1:
        out |= {"cs": pltpu.VMEM((c - 1, u3, 96, 128), BF16), "cr": pltpu.VMEM((c - 1, u3, 96, 128), BF16)}
        out |= {"c_sum": dma((2, c - 1)), "c_all": dma((2, c - 1))}
    return out


def remote(src, dst, send, recv, device):
    return pltpu.make_async_remote_copy(
        src_ref=src, dst_ref=dst, send_sem=send, recv_sem=recv, device_id={"dp": device}, device_id_type=MESH
    )


def first_row(kind, unit):
    return pl.multiple_of((unit // 16) * 48 if kind < 2 else (unit // 2) * 16, 16)


def row_count(kind, count):
    return count // 16 * 48 if kind < 2 else count // 2 * 16


def tiles(kind, unit, count, tile):
    row0 = first_row(kind, unit)
    blocks = count // 16 if kind < 2 else count // 2

    def body(q, _):
        if kind < 2:
            number, rest = q // (blocks * 4), lax.rem(q, blocks * 4)
            block, col0 = rest // 4, lax.rem(rest, 4) * 4
            rows = pl.ds(pl.multiple_of(row0 + block * 48, 16), 48)
            for col in range(4):
                lanes = pl.ds(pl.multiple_of((col0 + col) * 128, 128), 128)
                tile((number, rows, lanes), block * 16 + col0 + col, pl.ds(pl.multiple_of(number * 48, 16), 48))
        else:
            number, block = q // blocks, lax.rem(q, blocks)
            rows = pl.ds(pl.multiple_of(row0 + block * 16, 16), 16)
            for col in range(6):
                sub = pl.ds(pl.multiple_of(number * 48 + col % 3 * 16, 16), 16)
                tile((number, rows, slice(col * 128, (col + 1) * 128)), 2 * block + col // 3, sub)
        return 0

    lax.fori_loop(0, LAYERS * blocks * (4 if kind < 2 else 1), body, 0)


def piece_stages(kind, order, g, out, s, here, started):
    axes = [here.axes[name] for name in ORDERS[order]]
    a, b, c = sizes(order)
    u1, u2, u3 = UNITS // a, UNITS // a // b, UNITS // a // b // c
    rows = SHAPES[kind][0] // 2
    ia, ib, ic = (axis.at for axis in axes)
    base_b = ia * u1
    base_c = base_b + ib * u2
    base = base_c + ic * u3
    state = {}

    def go(key, copy):
        copy.start()
        started.append(copy.wait_send)
        state[key] = copy

    def begin():
        other = pl.multiple_of((1 - here.core) * rows, 16)
        mine = pl.multiple_of(here.core * rows, 16)
        for number in range(LAYERS):
            src, sem = g[number], s["core"].at[number]
            go(("core", number), remote(src.at[pl.ds(other, rows)], s["rec"].at[number], sem.at[0], sem.at[1], here.partner))
            state["own", number] = pltpu.make_async_copy(src.at[pl.ds(mine, rows)], s["own"].at[number], sem.at[2])
            state["own", number].start()

    def add_a(unit, count, arrived, dst, at):
        def tile(place, n, sub):
            x = s["own"][place].astype(F32) + s["rec"][place].astype(F32)
            for ref, skip in arrived:
                x = x + ref[skip + n, sub, :].astype(F32)
            dst[at + n, sub, :] = x.astype(dst.dtype)

        tiles(kind, unit, count, tile)

    def add_b(unit, count, arrived, dst, at):
        def body(n, _):
            x = s["acc1"][unit + n]
            for ref, skip in arrived:
                x = x + ref[skip + n].astype(F32)
            dst[at + n] = x.astype(dst.dtype)
            return 0

        lax.fori_loop(0, count, body, 0)

    def chain(name, axis, units, add, acc):
        n, steps, half = axis.n, axis.n // 2, units // 2

        def send(way, t):
            far = steps - t
            j = lax.rem(axis.at + (far if way == 0 else n - far), n)
            buf = s[name + "s"].at[way, t]
            got = s[name + "r"].at[way, t - 1] if t > 0 else None
            long, short = way * half, (1 - way) * half
            add(j * units + long, half, [(got, long)] if t > 0 else [], buf, long)
            if t > 0:
                add(j * units + short, half, [(got, short)] if t > 1 else [], buf, short)
                src, dst = buf, s[name + "r"].at[way, t]
            else:
                src, dst = buf.at[pl.ds(long, half)], s[name + "r"].at[way, t, pl.ds(long, half)]
            sem = s[name + "_sum"]
            go((name, way, t), remote(src, dst, sem.at[0, way, t], sem.at[1, way, t], axis.peer(1 if way == 0 else n - 1)))

        def start():
            if n == 1:
                add(0, units, [], acc, 0)
                return
            for way in range(2):
                send(way, 0)

        def step(t):
            for way in range(2):
                state[name, way, t].wait_recv()
                if t + 1 < steps:
                    send(way, t + 1)
            if t + 1 == steps:
                up, down = s[name + "r"].at[0, t], s[name + "r"].at[1, t]
                j = axis.at * units
                add(j, half, [(up, 0)] + ([(down, 0)] if t > 0 else []), acc, 0)
                add(j + half, half, [(down, half)] + ([(up, half)] if t > 0 else []), acc, half)

        return start, step

    def c_start():
        for d in range(1, c):
            j = lax.rem(ic + d, c)
            for k in range(u3):
                s["cs"][d - 1, k] = s["acc2"][j * u3 + k].astype(BF16)
            sem = s["c_sum"]
            go(("c", d), remote(s["cs"].at[d - 1], s["cr"].at[d - 1], sem.at[0, d - 1], sem.at[1, d - 1], axes[2].peer(d)))

    def c_step():
        for d in range(1, c):
            state["c", d].wait_recv()
        for k in range(u3):
            x = s["acc2"][ic * u3 + k]
            for d in range(1, c):
                x = x + s["cr"][d - 1, k].astype(F32)
            s["all"][base + k] = x.astype(BF16)

    def c_all_start():
        mine = s["all"].at[pl.ds(base, u3)]
        for d in range(1, c):
            sem = s["c_all"]
            go(("c_all", d), remote(mine, mine, sem.at[0, d - 1], sem.at[1, d - 1], axes[2].peer(d)))

    def c_all_step():
        for d in range(1, c):
            state["c_all", d].wait_recv()

    def spread(name, axis, units, first):
        n, steps, half = axis.n, axis.n // 2, units // 2

        def part(way, t, chunk):
            whole = t + 1 < steps
            return first + chunk * units + (0 if whole else way * half), units if whole else half

        def send(way, t):
            unit, count = part(way, t, lax.rem(axis.at + (n - t if way == 0 else t), n))
            ref, sem = s["all"].at[pl.ds(unit, count)], s[name + "_all"]
            go((name + "_all", way, t), remote(ref, ref, sem.at[0, way, t], sem.at[1, way, t], axis.peer(1 if way == 0 else n - 1)))

        def start():
            for way in range(2 if n > 1 else 0):
                send(way, 0)

        def step(t, then=None):
            for way in range(2):
                state[name + "_all", way, t].wait_recv()
                if t + 1 < steps:
                    send(way, t + 1)
            for way in range(2 if then else 0):
                unit, count = part(way, t, lax.rem(axis.at + (n - 1 - t if way == 0 else 1 + t), n))
                then(unit, count, 1 + way * steps + t)

        return start, step

    def finish(unit, count, slot):
        def tile(place, n, sub):
            s["own"][place] = s["all"][unit + n, sub, :]

        tiles(kind, unit, count, tile)
        row, many = first_row(kind, unit), row_count(kind, count)
        src = s["own"].at[:, pl.ds(row, many)]
        dst = out.at[:, pl.ds(pl.multiple_of(here.core * rows + row, 16), many)]
        copy = remote(src, dst, s["end"].at[0, slot], s["end"].at[1, slot], here.partner)
        local = pltpu.make_async_copy(src, dst, s["end"].at[2, slot])
        copy.start()
        local.start()
        started.extend([copy.wait_send, copy.wait_recv, local.wait])

    a_start, a_step = chain("a", axes[0], u1, add_a, s["acc1"])
    b_start, b_step = chain("b", axes[1], u2, add_b, s["acc2"])
    b_all_start, b_all_step = spread("b", axes[1], u2, base_b)
    a_all_start, a_all_step = spread("a", axes[0], u1, 0)

    def join(*parts):
        def run():
            for part in parts:
                part()

        return run

    def wait_core():
        for number in range(LAYERS):
            state["own", number].wait()
            state["core", number].wait_recv()

    def own_rows():
        finish(base_b, u1, 0)

    stages = [[wait_core, a_start]]
    times = [2.0]
    for t in range(a // 2):
        stages.append([functools.partial(a_step, t)])
        times.append({4: (12.0, 20.0)[t % 2], 8: 10.5}.get(a, 5.0))
    stages[-1].append(b_start)
    for t in range(b // 2):
        stages.append([functools.partial(b_step, t)])
        times.append(4.0)
    stages[-1].append(c_start)
    stages.append([c_step, c_all_start])
    times.append(4.5)
    stages.append([c_all_step, b_all_start])
    times.append(4.5)
    for t in range(b // 2):
        stages.append([functools.partial(b_all_step, t)])
        times.append(4.0)
    stages[-1] += [a_all_start, own_rows]
    for t in range(a // 2):
        stages.append([functools.partial(a_all_step, t, finish)])
        times.append({4: (20.0, 12.0)[t % 2], 8: 10.5}.get(a, 5.0))
    return begin, [(join(*stage), time) for stage, time in zip(stages, times)]


def sum_kernel(pieces, names, *refs):
    count = len(pieces)
    grads, refs = [refs[n * LAYERS : (n + 1) * LAYERS] for n in range(count)], refs[count * LAYERS :]
    outs, scratch = refs[:count], refs[count:]
    here = Place()
    barrier = pltpu.get_barrier_semaphore()
    axes = [here.axes[name] for name in "xyz"]
    peers = [here.partner] + [axis.peer(away) for axis in axes for away in range(1, axis.n)]
    for peer in peers:
        pl.semaphore_signal(barrier, inc=1, device_id={"dp": peer}, device_id_type=MESH)
    pl.semaphore_wait(barrier, len(peers))

    plan, started = [], []
    for n, (kind, order) in enumerate(pieces):
        s, scratch = dict(zip(names[n], scratch)), scratch[len(names[n]) :]
        begin, stages = piece_stages(kind, order, grads[n], outs[n], s, here, started)
        begin()
        when = 4.8 * n
        for stage, time in stages:
            when += time
            plan.append((when, len(plan), stage))
    for _, _, stage in sorted(plan, key=lambda entry: entry[:2]):
        stage()
    for wait in started:
        wait()


def group_sum(grads, pieces):
    specs = [piece_scratch(*piece) for piece in pieces]
    return pl.pallas_call(
        functools.partial(sum_kernel, pieces, [tuple(spec) for spec in specs]),
        out_shape=[jax.ShapeDtypeStruct((LAYERS, *SHAPES[kind]), BF16) for kind, _ in pieces],
        in_specs=[pl.BlockSpec(memory_space=pl.ANY)] * len(pieces) * LAYERS,
        out_specs=[pl.BlockSpec(memory_space=pl.ANY)] * len(pieces),
        scratch_shapes=[shape for spec in specs for shape in spec.values()],
        compiler_params=pltpu.CompilerParams(collective_id=0, has_side_effects=True, vmem_limit_bytes=63 * 2**20),
        cost_estimate=pl.CostEstimate(flops=300_000_000, bytes_accessed=60_000_000, transcendentals=0),
        name="group_sum",
    )(*itertools.chain(*grads))


def adamw(w, m, v, g):
    m = 0.9 * m + 0.1 * g
    v = 0.95 * v + 0.05 * g * g
    step = m * lax.rsqrt(v + 1e-8) + 0.1 * w
    return (w - 0.02 * step).astype(jnp.bfloat16), m, v


def solution(mesh):
    def step(x, dy, *arrays):
        weights, m, v = (arrays[i : i + 3] for i in (0, 3, 6))
        layers = weights[0].shape[0]
        h, kept = x[0], []
        for number in range(layers):
            kept.append(h)
            h = layer(h, {name: w[number] for name, w in zip(NAMES, weights, strict=True)})
        by_h, grads = dy[0], {}
        for number in reversed(range(layers)):
            _, back = jax.vjp(lambda w, h: layer(h, w), {name: w[number] for name, w in zip(NAMES, weights, strict=True)}, kept[number])
            by_w, by_h = back(by_h)
            for kind, name in enumerate(NAMES):
                grads[number, kind] = by_w[name]
        summed = group_sum([[grads[number, kind] for number in range(layers)] for kind, _ in PIECES], PIECES)
        summed = {kind: g for (kind, _), g in zip(PIECES, summed, strict=True)}
        gradients = [summed[kind].astype(F32) for kind in range(3)]
        new = [adamw(w.astype(F32), m, v, g) for w, m, v, g in zip(weights, m, v, gradients, strict=True)]
        return tuple(one[which] for which in range(3) for one in new)

    return jax.shard_map(
        step,
        mesh=mesh,
        in_specs=(P(("rep", "dp"), None, None),) * 2 + (P(None, None, None),) * 9,
        out_specs=(P("rep", None, None),) * 9,
        check_vma=False,
    )
```
